768 devices in a mesh: space: 32 (over y, x), tm: 24 (over z, core).
Axes of the slice: x: 4, y: 8, z: 12, core: 2. Of those that a mesh axis runs over, the one named last changes fastest.
Arguments:
- links: float32 [24, 3, 2, 3, 3, 64, 4096], P('tm', None, None, None, None, 'space'), may hold values from -1 to 1, as said below
- propagator: float32 [2, 144, 64, 4096], P(None, 'tm', 'space'), may hold values from -6 to 6
- sink_time: int32 [1], replicated, may hold values from 0 to 98303
- src_time: int32 [1], replicated, may hold values from 0 to 98303
- src_site: int32 [1], replicated, may hold values from 0 to 262143
Outputs:
- fixed_links: float32 [24, 3, 2, 3, 3, 64, 4096], P('tm', None, None, None, None, 'space')
- wall: float32 [2, 144], replicated
The draws below stay inside these ranges and needn't reach their ends.
Inputs may be any that keep to these rules, and one draw needn't show every extreme that they name: `links`: every link is a special unitary 3 x 3 matrix up to rounding.
All inputs are finite; a program needn't handle non-finite values.
Results may differ from the reference program's by a relative error of at most 0.0001.
Values sent between devices are 32-bit elements; how exact they have to be, the bound alone decides.
A program may use at most 128 MiB of HBM per device.

```python
import math
import jax
import jax.numpy as jnp
from jax import lax

L = 64
SC = 12
ITERS = 2
NX = 64
NT = 24


def draw_product(left_matrix, right_matrix):
    pattern = 'tdikxn,tdkjxn->tdijxn'
    real_part = jnp.einsum(pattern, left_matrix[:, :, 0], right_matrix[:, :, 0]) - jnp.einsum(pattern, left_matrix[:, :, 1], right_matrix[:, :, 1])
    imag_part = jnp.einsum(pattern, left_matrix[:, :, 0], right_matrix[:, :, 1]) + jnp.einsum(pattern, left_matrix[:, :, 1], right_matrix[:, :, 0])
    return jnp.stack([real_part, imag_part], axis=2)


def draw_links(key, part):
    normal_draw = jax.random.normal(key, (NT, 3, 2, 3, 3, NX, L * L), jnp.float32)
    real_part = normal_draw[:, :, 0]
    imag_part = normal_draw[:, :, 1]
    real_anti = 0.5 * (real_part - jnp.swapaxes(real_part, 2, 3))
    imag_sym = 0.5 * (imag_part + jnp.swapaxes(imag_part, 2, 3))
    trace_third = (imag_sym[:, :, 0, 0] + imag_sym[:, :, 1, 1] + imag_sym[:, :, 2, 2]) / 3.0
    unit_matrix = jnp.eye(3, dtype=jnp.float32)[None, None, :, :, None, None]
    imag_sym = imag_sym - unit_matrix * trace_third[:, :, None, None]
    algebra = jnp.stack([real_anti, imag_sym], axis=2) / 16.0
    identity = jnp.stack([jnp.broadcast_to(unit_matrix, real_anti.shape), jnp.zeros(real_anti.shape, jnp.float32)], axis=2)
    result = identity
    for degree in range(8, 0, -1):
        result = identity + draw_product(algebra, result) / degree
    for square_index in range(4):
        result = draw_product(result, result)
    return result


def level_of(rng, extent, shards, least, largest):
    def one(axis_at, shards_of):
        heights = jax.random.uniform(jax.random.fold_in(jax.random.fold_in(rng, 6), axis_at), (shards_of,), jnp.float32, least / len(shards), largest / len(shards))
        return jnp.repeat(jnp.exp(heights), extent[axis_at] // shards_of).reshape((-1,) + (1,) * (len(extent) - axis_at - 1))

    level = one(*shards[0])
    for cut in shards[1:]:
        level = level * one(*cut)
    return level


def noise(key, shape, scale, reach, cuts=(), kind=jnp.bfloat16):
    entries = scale * jax.random.normal(key, shape, jnp.float32)
    if cuts:
        entries = entries * level_of(key, shape, cuts, -0.22, 0.18)
    return jnp.clip(entries, -reach, reach).astype(kind)


def setup_inputs(seed: int = 0) -> dict:
    arg_keys = jax.random.split(jax.random.key(seed), 6)
    links = draw_links(jax.random.fold_in(arg_keys[5], 71), 0)
    propagator = noise(arg_keys[1], (2, SC * SC, NX, L * L), 1.0, 6.0, ((1, 24), (2, 32)), jnp.float32)
    sink_time = jax.random.randint(arg_keys[2], (1,), 0, NT * 4096).astype(jnp.int32)
    src_time = jax.random.randint(arg_keys[3], (1,), 0, NT * 4096).astype(jnp.int32)
    src_site = jax.random.randint(arg_keys[4], (1,), 0, NX * L * L).astype(jnp.int32)
    return dict(links=links, propagator=propagator, sink_time=sink_time, src_time=src_time, src_site=src_site)


STEP_SIZE = 0.08
PEAK_SQUARE = 12.0
ENTRY_PAIRS = ((0, 0), (0, 1), (0, 2), (1, 1), (1, 2), (2, 2))
EXACT = lax.Precision.HIGHEST


def colour_product(left_matrix, right_matrix):
    return jnp.sum(left_matrix[:, :, None] * right_matrix[None, :, :], axis=1)


def complex_product(left_matrix, right_matrix):
    real_part = colour_product(left_matrix[0], right_matrix[0]) - colour_product(left_matrix[1], right_matrix[1])
    imag_part = colour_product(left_matrix[0], right_matrix[1]) + colour_product(left_matrix[1], right_matrix[0])
    return jnp.stack([real_part, imag_part])


def dagger(matrix):
    return jnp.stack([jnp.swapaxes(matrix[0], 0, 1), -jnp.swapaxes(matrix[1], 0, 1)])


def roll_depth(values, amount):
    old_shape = values.shape
    folded = values.reshape(old_shape[:-1] + (L, L))
    return jnp.roll(folded, amount, axis=-1).reshape(old_shape)


def project(divergence):
    real_part = 0.5 * (divergence[0] - jnp.swapaxes(divergence[0], 0, 1))
    imag_part = 0.5 * (divergence[1] + jnp.swapaxes(divergence[1], 0, 1))
    trace_third = (imag_part[0, 0] + imag_part[1, 1] + imag_part[2, 2]) / 3.0
    real_six = jnp.stack([real_part[row_index, column_index] for row_index, column_index in ENTRY_PAIRS])
    imag_six = jnp.stack([imag_part[row_index, column_index] - trace_third if row_index == column_index else imag_part[row_index, column_index] for row_index, column_index in ENTRY_PAIRS])
    return real_six, imag_six


def assemble(real_six, imag_six):
    zero_plane = jnp.zeros_like(real_six[0])
    position = {}
    for entry_index, entry_pair in enumerate(ENTRY_PAIRS):
        position[entry_pair] = entry_index
    real_rows = []
    imag_rows = []
    for row_index in range(3):
        real_line = []
        imag_line = []
        for column_index in range(3):
            if row_index == column_index:
                real_line.append(zero_plane)
                imag_line.append(imag_six[position[(row_index, row_index)]])
            elif row_index < column_index:
                slot_index = position[(row_index, column_index)]
                real_line.append(real_six[slot_index])
                imag_line.append(imag_six[slot_index])
            else:
                slot_index = position[(column_index, row_index)]
                real_line.append(-real_six[slot_index])
                imag_line.append(imag_six[slot_index])
        real_rows.append(jnp.stack(real_line))
        imag_rows.append(jnp.stack(imag_line))
    return jnp.stack([jnp.stack(real_rows), jnp.stack(imag_rows)])


def exponential(algebra):
    unit_matrix = jnp.eye(3, dtype=jnp.float32).reshape((3, 3) + (1,) * (algebra.ndim - 3))
    identity = jnp.stack([jnp.broadcast_to(unit_matrix, algebra.shape[1:]), jnp.zeros(algebra.shape[1:], jnp.float32)])
    result = identity
    for degree in range(6, 0, -1):
        result = identity + complex_product(algebra, result) / degree
    for square_index in range(3):
        result = complex_product(result, result)
    return result


def rotate(lattice, gauge_field, gauge_ahead):
    along_x = complex_product(complex_product(gauge_field, lattice[0]), dagger(gauge_ahead))
    along_y = complex_product(complex_product(gauge_field, lattice[1]), dagger(jnp.roll(gauge_field, -L, axis=4)))
    along_z = complex_product(complex_product(gauge_field, lattice[2]), dagger(roll_depth(gauge_field, -1)))
    return jnp.stack([along_x, along_y, along_z])


def sink_product(gauge_field, propagator):
    pair_count = propagator.shape[1]
    source = propagator.reshape((2, pair_count // 3, 3) + propagator.shape[2:])
    pattern = "acxn,qcxn->qa"
    real_part = jnp.einsum(pattern, gauge_field[0], source[0], precision=EXACT) - jnp.einsum(pattern, gauge_field[1], source[1], precision=EXACT)
    imag_part = jnp.einsum(pattern, gauge_field[0], source[1], precision=EXACT) + jnp.einsum(pattern, gauge_field[1], source[0], precision=EXACT)
    return jnp.stack([real_part.reshape(pair_count), imag_part.reshape(pair_count)])


def source_rotate(wall_total, anchor):
    by_spin = wall_total.reshape(2, 4, 3, SC)
    pattern = "scn,bc->sbn"
    real_part = jnp.einsum(pattern, by_spin[0], anchor[0], precision=EXACT) + jnp.einsum(pattern, by_spin[1], anchor[1], precision=EXACT)
    imag_part = jnp.einsum(pattern, by_spin[1], anchor[0], precision=EXACT) - jnp.einsum(pattern, by_spin[0], anchor[1], precision=EXACT)
    return jnp.stack([real_part.reshape(SC * SC), imag_part.reshape(SC * SC)])


def sine_squares(length):
    wavenumber = jnp.arange(length, dtype=jnp.float32)
    return 4.0 * jnp.sin(math.pi * wavenumber / length) ** 2


def inverse_square():
    across = sine_squares(NX)
    sine_square = sine_squares(L)
    momentum = across[:, None, None] + sine_square[None, :, None] + sine_square[None, None, :]
    guarded = jnp.where(momentum > 0.0, momentum, 1.0)
    return jnp.where(momentum > 0.0, PEAK_SQUARE / guarded, 0.0)


def reference(links, propagator, sink_time, src_time, src_site):
    filter_weight = inverse_square()

    def fix_timeslice(lattice):
        overall = None
        for sweep_index in range(ITERS):
            divergence = jnp.roll(lattice[0], 1, axis=3) - lattice[0] + jnp.roll(lattice[1], L, axis=4) - lattice[1] + roll_depth(lattice[2], 1) - lattice[2]
            real_six, imag_six = project(divergence)
            packed = (real_six + 1j * imag_six).reshape(6, NX, L, L)
            spectrum = jnp.fft.fftn(packed, axes=(1, 2, 3)) * filter_weight[None]
            filtered = jnp.fft.ifftn(spectrum, axes=(1, 2, 3)).reshape(6, NX, L * L)
            algebra = assemble(jnp.real(filtered), jnp.imag(filtered))
            gauge_field = exponential(algebra * (STEP_SIZE / 16.0))
            lattice = rotate(lattice, gauge_field, jnp.roll(gauge_field, -1, axis=3))
            overall = gauge_field if overall is None else complex_product(gauge_field, overall)
        return lattice, overall

    fixed_links, overall_all = lax.map(fix_timeslice, links)
    sink_slice = sink_time[0] % NT
    source_slice = src_time[0] % NT
    wall_total = sink_product(overall_all[sink_slice], propagator)
    site_index = src_site[0]
    anchor = overall_all[source_slice][:, :, :, site_index // (L * L), site_index % (L * L)]
    wall = source_rotate(wall_total, anchor) * float(NX * L * L) ** -0.5
    return fixed_links, wall
```

```python
import functools

import jax
import jax.numpy as jnp
import ml_dtypes
import numpy as np
from jax import lax
from jax.experimental import pallas as pl
from jax.experimental.pallas import tpu as pltpu
from jax.sharding import PartitionSpec as P

L = 64
SC = 12
ITERS = 2
STEP_SIZE = 0.08
PEAK_SQUARE = 12.0
ROWS = 32
PART = 24
SHARE = 24
F32 = jnp.float32
BF16 = jnp.bfloat16
MESH = pl.DeviceIdType.MESH


def halves(table):
    table = np.asarray(table, np.float32)
    high = table.astype(ml_dtypes.bfloat16)
    low = (table - high.astype(np.float32)).astype(ml_dtypes.bfloat16)
    return high, low


def left_table(table):
    high, low = halves(table)
    return np.concatenate([high, high, low], axis=1)


def right_table(table):
    high, low = halves(table)
    return np.concatenate([high, low], axis=0)


def tables(space_count):
    turn = 2.0 * np.pi
    short = np.arange(ROWS)
    angle = turn * (np.outer(short, short) % ROWS) / ROWS
    cosine, sine = np.cos(angle), np.sin(angle)
    row_forward = np.block([[cosine, sine], [-sine, cosine]])
    row_back = np.block([[cosine, -sine], [sine, cosine]])
    lane = np.arange(128)
    half, deep = lane // L, lane % L
    sign = np.where(np.outer(half, half) % 2 == 1, -1.0, 1.0)
    angle = turn * (np.outer(deep, deep) % L) / L
    cosine, sine = sign * np.cos(angle), sign * np.sin(angle)
    lane_forward = np.block([[cosine, -sine], [sine, cosine]])
    lane_back = np.block([[cosine, sine], [-sine, cosine]])
    angle = turn * np.outer(short, half) / L
    twist = np.stack([np.cos(angle), np.sin(angle)]).astype(np.float32)
    wave = np.arange(L)
    place = np.concatenate([(2 * np.arange(space_count) + plane) % L for plane in range(3)])
    angle = turn * (np.outer(wave, place) % L) / L
    cosine, sine = np.cos(angle), np.sin(angle)
    across_forward = np.block([[cosine, sine], [-sine, cosine]])
    across_back = np.block([[cosine.T, -sine.T], [sine.T, cosine.T]])
    square = 4.0 * np.sin(np.pi * wave / L) ** 2
    square_across = np.broadcast_to(square[:, None], (L, 128)).astype(np.float32)
    square_block = np.stack(
        [square[block + 32 * half] + square[deep] for block in range(space_count)]
    ).astype(np.float32)
    return (
        left_table(row_forward),
        left_table(row_back),
        right_table(lane_forward),
        right_table(lane_back),
        left_table(across_forward),
        left_table(across_back),
        twist,
        square_across,
        square_block[:, None, :],
    )


def dot(left, right):
    return lax.dot_general(left, right, (((1,), (0,)), ((), ())), preferred_element_type=F32)


def split(values):
    high = values.astype(BF16)
    return high, (values - high.astype(F32)).astype(BF16)


def table_times(table, values):
    high, low = split(values)
    return dot(table, jnp.concatenate([high, low, high], axis=0))


def times_table(values, table):
    size = table.shape[0] // 2
    high, low = split(values)
    upper = table[:size]
    return dot(high, upper) + dot(high, table[size:]) + dot(low, upper)


def c_mul(left, right):
    return (
        left[0] * right[0] - left[1] * right[1],
        left[0] * right[1] + left[1] * right[0],
    )


def matrix_product(left, right):
    out = []
    for row in range(3):
        line = []
        for column in range(3):
            real, imag = None, None
            for inner in range(3):
                lr, li = left[row][inner]
                rr, ri = right[inner][column]
                real_term = lr * rr - li * ri
                imag_term = lr * ri + li * rr
                real = real_term if real is None else real + real_term
                imag = imag_term if imag is None else imag + imag_term
            line.append((real, imag))
        out.append(line)
    return out


def product_dagger(left, right):
    turned = [[(right[c][r][0], -right[c][r][1]) for c in range(3)] for r in range(3)]
    out = []
    for row in range(3):
        line = []
        for column in range(3):
            real, imag = None, None
            for inner in range(3):
                lr, li = left[row][inner]
                rr, ri = right[column][inner]
                real_term = lr * rr + li * ri
                imag_term = li * rr - lr * ri
                real = real_term if real is None else real + real_term
                imag = imag_term if imag is None else imag + imag_term
            line.append((real, imag))
        out.append(line)
    del turned
    return out


def rotation_of(fields):
    x01, x02, x12 = (fields[0], fields[4]), (fields[1], fields[5]), (fields[2], fields[6])
    d0, d1 = fields[3], fields[7]
    d2 = -(d0 + d1)
    n01 = x01[0] * x01[0] + x01[1] * x01[1]
    n02 = x02[0] * x02[0] + x02[1] * x02[1]
    n12 = x12[0] * x12[0] + x12[1] * x12[1]
    s0, s1, s2 = d0 * d0, d1 * d1, d2 * d2
    t = -(0.5 * (s0 + s1 + s2) + (n01 + n02 + n12))
    pair = c_mul(x01, x12)
    imag_w = pair[1] * x02[0] - pair[0] * x02[1]
    e = d0 * n12 + d1 * n02 + d2 * n01 - d0 * d1 * d2 - 2.0 * imag_w
    y01 = (
        d2 * x01[1] - (x02[0] * x12[0] + x02[1] * x12[1]),
        -d2 * x01[0] - (x02[1] * x12[0] - x02[0] * x12[1]),
    )
    y02 = (d1 * x02[1] + pair[0], -d1 * x02[0] + pair[1])
    y12 = (
        d0 * x12[1] - (x01[0] * x02[0] + x01[1] * x02[1]),
        -d0 * x12[0] - (x01[0] * x02[1] - x01[1] * x02[0]),
    )
    q0, q1, q2 = -(s0 + n01 + n02), -(s1 + n01 + n12), -(s2 + n02 + n12)
    a = (jnp.ones_like(t), e * (1.0 / 120.0))
    b = ((1.0 + t * (1.0 / 30.0)) * 0.25, jnp.zeros_like(t))
    c = (jnp.full_like(t, 0.05), jnp.zeros_like(t))
    for degree in (3, 2, 1):
        scale = 1.0 / degree
        a, b, c = (
            (1.0 - e * c[1] * scale, e * c[0] * scale),
            ((a[0] + c[0] * t) * scale, (a[1] + c[1] * t) * scale),
            (b[0] * scale, b[1] * scale),
        )
    for _ in range(3):
        aa, bb, cc = c_mul(a, a), c_mul(b, b), c_mul(c, c)
        ab, ac, bc = c_mul(a, b), c_mul(a, c), c_mul(b, c)
        a, b, c = (
            (aa[0] - 2.0 * e * bc[1], aa[1] + 2.0 * e * bc[0]),
            (
                2.0 * (ab[0] + t * bc[0]) - e * cc[1],
                2.0 * (ab[1] + t * bc[1]) + e * cc[0],
            ),
            (2.0 * ac[0] + bb[0] + t * cc[0], 2.0 * ac[1] + bb[1] + t * cc[1]),
        )
    out = [[None] * 3 for _ in range(3)]
    for at, (d, q) in enumerate(((d0, q0), (d1, q1), (d2, q2))):
        out[at][at] = (a[0] - b[1] * d + c[0] * q, a[1] + b[0] * d + c[1] * q)
    for row, column, x, y in ((0, 1, x01, y01), (0, 2, x02, y02), (1, 2, x12, y12)):
        p1, p2, p3, p4 = b[0] * x[0], b[1] * x[1], b[0] * x[1], b[1] * x[0]
        r1, r2, r3, r4 = c[0] * y[0], c[1] * y[1], c[0] * y[1], c[1] * y[0]
        out[row][column] = (p1 - p2 + r1 - r2, p3 + p4 + r3 + r4)
        out[column][row] = (r1 + r2 - p1 - p2, p3 - p4 - r3 + r4)
    return out


def entry(row, column):
    return row * 3 + column


def kernel(
    space_count,
    time_count,
    sink_time,
    src_time,
    src_site,
    links_in,
    prop_in,
    row_forward,
    row_back,
    lane_forward,
    lane_back,
    across_forward,
    across_back,
    twist,
    square_across,
    square_block,
    links_out,
    rows_out,
    lk,
    pr,
    send,
    recv,
    algebra,
    gauge,
    ahead_y,
    half_in,
    stage,
    share_in,
    shared,
    full,
    lines,
    line,
    line_in,
    total_line,
    total_in,
    copy_sem,
    a2a_send,
    a2a_recv,
    half_sem,
    one_send,
    one_recv,
    two_send,
    two_recv,
    swap_sem,
    line_send,
    line_recv,
    last_send,
    last_recv,
):
    me = lax.axis_index("space")
    my_time = lax.axis_index("tm")
    depth_count = time_count // 2
    my_depth = my_time // 2
    my_core = my_time % 2
    partner = my_time + 1 - 2 * my_core
    sink_slice = lax.rem(sink_time[0], time_count)
    source_slice = lax.rem(src_time[0], time_count)
    sink_depth = sink_slice // 2
    sink_core = sink_slice - 2 * sink_depth

    load_links = pltpu.make_async_copy(links_in, lk, copy_sem.at[0])
    load_links.start()
    load_prop = pltpu.make_async_copy(prop_in, pr, copy_sem.at[1])
    load_prop.start()

    barrier = pltpu.get_barrier_semaphore()

    def greet_space(step, carry):
        peer = lax.rem(me + step, space_count)
        pl.semaphore_signal(barrier, inc=1, device_id={"space": peer}, device_id_type=MESH)
        return carry

    def greet_time(step, carry):
        peer = lax.rem(my_time + step, time_count)
        pl.semaphore_signal(barrier, inc=1, device_id={"tm": peer}, device_id_type=MESH)
        return carry

    lax.fori_loop(1, space_count, greet_space, 0)
    lax.fori_loop(1, time_count, greet_time, 0)

    lane_at = lax.broadcasted_iota(jnp.int32, (ROWS, 128), 1)
    row_at = lax.broadcasted_iota(jnp.int32, (ROWS, 128), 0)
    first_half = lane_at < L
    deep_at = lane_at % L
    deep_chunk = lax.broadcasted_iota(jnp.int32, (8, 128), 1) % L
    deep_last = deep_chunk == L - 1

    def from_lower_y(values):
        turned = pltpu.roll(values, L, 1)
        return jnp.where(first_half, pltpu.roll(turned, 1, 0), turned)

    def from_upper_y(values):
        turned = pltpu.roll(values, L, 1)
        return jnp.where(first_half, turned, pltpu.roll(turned, ROWS - 1, 0))

    def from_lower_z(values):
        return jnp.where(deep_at == 0, pltpu.roll(values, L + 1, 1), pltpu.roll(values, 1, 1))

    def chunk_upper_z(values):
        return jnp.where(deep_last, pltpu.roll(values, L - 1, 1), pltpu.roll(values, 127, 1))

    def projected(direction, plane):
        def one(part, row, column):
            start = ((direction * 2 + part) * 9 + entry(row, column)) * L + plane
            return lk[pl.ds(start, ROWS, stride=2), :]

        real, imag = [], []
        for row, column in ((0, 1), (0, 2), (1, 2)):
            real.append(0.5 * (one(0, row, column) - one(0, column, row)))
            imag.append(0.5 * (one(1, row, column) + one(1, column, row)))
        diagonal = [one(1, at, at) for at in range(3)]
        third = (diagonal[0] + diagonal[1] + diagonal[2]) * (1.0 / 3.0)
        real.append(diagonal[0] - third)
        imag.append(diagonal[1] - third)
        return real + imag

    def exchange(round_index, step):
        peer = lax.rem(me + step, space_count)
        return pltpu.make_async_remote_copy(
            src_ref=send.at[round_index, pl.ds(pl.multiple_of(peer * PART, 8), PART), :],
            dst_ref=recv.at[round_index, pl.ds(pl.multiple_of(me * PART, 8), PART), :],
            send_sem=a2a_send.at[round_index, step],
            recv_sem=a2a_recv.at[round_index, me],
            device_id={"space": peer},
            device_id_type=MESH,
        )

    def exchange_arrival(round_index, step):
        peer = lax.rem(me + step, space_count)
        return pltpu.make_async_remote_copy(
            src_ref=send.at[round_index, pl.ds(pl.multiple_of(peer * PART, 8), PART), :],
            dst_ref=recv.at[round_index, pl.ds(pl.multiple_of(peer * PART, 8), PART), :],
            send_sem=a2a_send.at[round_index, step],
            recv_sem=a2a_recv.at[round_index, peer],
            device_id={"space": peer},
            device_id_type=MESH,
        )

    def start_exchange(round_index):
        def begin(step, carry):
            exchange(round_index, step).start()
            return carry

        lax.fori_loop(1, space_count, begin, 0)
        own = pl.ds(pl.multiple_of(me * PART, 8), PART)
        recv[round_index, own, :] = send[round_index, own, :]

    def end_exchange(round_index):
        def finish(step, carry):
            arrival = exchange_arrival(round_index, step)
            arrival.wait_send()
            arrival.wait_recv()
            return carry

        lax.fori_loop(1, space_count, finish, 0)

    def block_rows(plane, part, field):
        return pl.ds(plane * 8 + part * 4 + field, space_count, stride=PART)

    def spread(sweep):
        nothing = [jnp.zeros((ROWS, 128), F32)] * 8
        fields = []
        along_x = [projected(0, plane) for plane in range(2)]
        for plane in range(2):
            along_y, along_z = projected(1, plane), projected(2, plane)
            behind = nothing if plane == 0 else along_x[0]
            fields.append(
                [
                    behind[at]
                    - along_x[plane][at]
                    + (from_lower_y(along_y[at]) - along_y[at])
                    + (from_lower_z(along_z[at]) - along_z[at])
                    for at in range(8)
                ]
            )
        fields.append(along_x[1])
        wide = [
            jnp.concatenate(
                [fields[plane][part * 4 + at] for plane in range(3) for at in range(4)], axis=1
            )
            for part in range(2)
        ]
        turned = table_times(row_forward[...], jnp.concatenate(wide, axis=0))
        cosine, sine = twist[0], twist[1]
        lines_in = []
        for block in range(12):
            real = turned[:ROWS, block * 128 : (block + 1) * 128]
            imag = turned[ROWS:, block * 128 : (block + 1) * 128]
            lines_in.append(
                jnp.concatenate([real * cosine + imag * sine, imag * cosine - real * sine], axis=1)
            )
        spectrum = times_table(jnp.concatenate(lines_in, axis=0), lane_forward)
        for plane in range(3):
            for part in range(2):
                for field in range(4):
                    at = (plane * 4 + field) * ROWS
                    send[2 * sweep, block_rows(plane, part, field), :] = spectrum[
                        at : at + ROWS, part * 128 : (part + 1) * 128
                    ]

    def across(sweep):
        gathered = jnp.concatenate(
            [
                jnp.concatenate(
                    [recv[2 * sweep, block_rows(plane, part, field), :] for field in range(4)],
                    axis=1,
                )
                for part in range(2)
                for plane in range(3)
            ],
            axis=0,
        )
        spectrum = table_times(across_forward[...], gathered)
        momentum = square_across[...] + square_block[me]
        inside = momentum > 0.0
        factor = PEAK_SQUARE * (STEP_SIZE / 16.0) / float(L) ** 3
        weight = jnp.where(inside, factor / jnp.where(inside, momentum, 1.0), 0.0)
        weight = jnp.concatenate([jnp.concatenate([weight] * 4, axis=1)] * 2, axis=0)
        back = table_times(across_back[...], spectrum * weight)
        for part in range(2):
            for plane in range(3):
                for field in range(4):
                    at = (part * 3 + plane) * ROWS
                    send[2 * sweep + 1, block_rows(plane, part, field), :] = back[
                        at : at + ROWS, field * 128 : (field + 1) * 128
                    ]

    def algebra_rows(plane, part, field):
        if plane == 2:
            return 512 + (part * 4 + field) * ROWS
        return part * 256 + (plane * 4 + field) * ROWS

    def gather_back(sweep):
        lines_in = jnp.concatenate(
            [
                jnp.concatenate(
                    [recv[2 * sweep + 1, block_rows(plane, part, field), :] for part in range(2)],
                    axis=1,
                )
                for plane in range(3)
                for field in range(4)
            ],
            axis=0,
        )
        turned = times_table(lines_in, lane_back)
        cosine, sine = twist[0], twist[1]
        reals, imags = [], []
        for block in range(12):
            real = turned[block * ROWS : (block + 1) * ROWS, :128]
            imag = turned[block * ROWS : (block + 1) * ROWS, 128:]
            reals.append(real * cosine - imag * sine)
            imags.append(imag * cosine + real * sine)
        wide = jnp.concatenate(
            [jnp.concatenate(reals, axis=1), jnp.concatenate(imags, axis=1)], axis=0
        )
        sites = table_times(row_back[...], wide)
        for plane in range(3):
            for part in range(2):
                for field in range(4):
                    block = plane * 4 + field
                    start = algebra_rows(plane, part, field)
                    algebra[sweep, start : start + ROWS, :] = sites[
                        part * ROWS : (part + 1) * ROWS, block * 128 : (block + 1) * 128
                    ]

    def exponentials(sweep):
        def one(step, carry):
            plane, row = step // 4, pl.multiple_of((step % 4) * 8, 8)
            base = jnp.where(plane == 2, 512, plane * 128)
            stride = jnp.where(plane == 2, 128, 256)
            fields = []
            for part in range(2):
                for field in range(4):
                    start = pl.multiple_of(base + part * stride + field * ROWS + row, 8)
                    fields.append(algebra[sweep, pl.ds(start, 8), :])
            matrix = rotation_of(fields)
            for part in range(2):
                for a in range(3):
                    for b in range(3):
                        gauge[plane, part * 9 + entry(a, b), pl.ds(row, 8), :] = matrix[a][b][part]
            return carry

        lax.fori_loop(0, 12, one, 0)

        def shift(plane, carry):
            for at in range(18):
                ahead_y[plane, at] = from_upper_y(gauge[plane, at])
            return carry

        lax.fori_loop(0, 2, shift, 0)

    def matrix_at(read):
        return [[(read(entry(a, b)), read(9 + entry(a, b))) for b in range(3)] for a in range(3)]

    def rotate_links():
        def one(step, carry):
            plane, chunk = step // 4, step % 4
            row = pl.multiple_of(chunk * 8, 8)
            here = matrix_at(lambda at: gauge[plane, at, pl.ds(row, 8), :])
            for direction in range(3):
                if direction == 0:
                    ahead = matrix_at(lambda at: gauge[plane + 1, at, pl.ds(row, 8), :])
                elif direction == 1:
                    ahead = matrix_at(lambda at: ahead_y[plane, at, pl.ds(row, 8), :])
                else:
                    ahead = [[tuple(chunk_upper_z(v) for v in pair) for pair in r] for r in here]

                def rows(at):
                    start = (direction * 18 + at) * L
                    return pl.ds(start + 16 * chunk + plane, 8, stride=2)

                link = matrix_at(lambda at: lk[rows(at), :])
                moved = product_dagger(matrix_product(here, link), ahead)
                for part in range(2):
                    for a in range(3):
                        for b in range(3):
                            lk[rows(part * 9 + entry(a, b)), :] = moved[a][b][part]
            return carry

        lax.fori_loop(0, 8, one, 0)

    plane_index = src_site[0] // (L * L) - 2 * me
    column_index = lax.rem(src_site[0], L * L)
    wanted = jnp.where(source_slice == my_time, plane_index * (L * L) + column_index, -1)

    def anchor_lines(sweep):
        site = row_at * 128 + lane_at
        for at in range(18):
            picked = jnp.where(site == wanted, gauge[0, at], 0.0) + jnp.where(
                site + L * L == wanted, gauge[1, at], 0.0
            )
            place = 12 + 18 * sweep + at
            lines[place : place + 1, :] = jnp.sum(picked, axis=0, keepdims=True)

    def half_copy(sweep):
        return pltpu.make_async_remote_copy(
            src_ref=algebra.at[sweep, pl.ds(pl.multiple_of((1 - my_core) * 256, 8), 256), :],
            dst_ref=half_in.at[sweep],
            send_sem=half_sem.at[sweep, 0],
            recv_sem=half_sem.at[sweep, 1],
            device_id={"tm": partner},
            device_id_type=MESH,
        )

    def share_copy(sweep, step, arrival):
        depth = lax.rem(my_depth + step, depth_count)
        landing = depth if arrival else my_depth
        return pltpu.make_async_remote_copy(
            src_ref=stage.at[sweep, depth],
            dst_ref=share_in.at[sweep, landing],
            send_sem=one_send.at[sweep, step],
            recv_sem=one_recv.at[sweep, landing],
            device_id={"tm": depth * 2 + my_core},
            device_id_type=MESH,
        )

    def shared_copy(sweep, step, arrival):
        depth = lax.rem(my_depth + step, depth_count)
        landing = depth if arrival else my_depth
        return pltpu.make_async_remote_copy(
            src_ref=shared.at[sweep],
            dst_ref=full.at[sweep, my_core, landing],
            send_sem=two_send.at[sweep, step],
            recv_sem=two_recv.at[sweep, landing],
            device_id={"tm": depth * 2 + my_core},
            device_id_type=MESH,
        )

    def swap_copy(sweep, arrival):
        core = 1 - my_core if arrival else my_core
        return pltpu.make_async_remote_copy(
            src_ref=full.at[sweep, my_core],
            dst_ref=full.at[sweep, core],
            send_sem=swap_sem.at[sweep, 0],
            recv_sem=swap_sem.at[sweep, 1],
            device_id={"tm": partner},
            device_id_type=MESH,
        )

    def each_depth(action):
        def one(step, carry):
            action(step)
            return carry

        lax.fori_loop(1, depth_count, one, 0)

    def sink_start(sweep):
        half_copy(sweep).start()

    def sink_shares(sweep):
        half_copy(sweep).wait()
        mine = algebra[sweep, pl.ds(pl.multiple_of(my_core * 256, 8), 256), :]
        chosen = jnp.where(sink_core == my_core, mine, half_in[sweep])
        for at in range(depth_count):
            low, high = at * SHARE, min((at + 1) * SHARE, 256)
            if high > low:
                stage[sweep, at, : high - low, :] = chosen[low:high]
            filled = max(high - low, 0)
            if filled < SHARE:
                stage[sweep, at, filled:, :] = jnp.zeros((SHARE - filled, 128), F32)
        each_depth(lambda step: share_copy(sweep, step, False).start())
        share_in[sweep, my_depth] = stage[sweep, my_depth]

    def wait_both(copy):
        copy.wait_send()
        copy.wait_recv()

    def sink_shared(sweep):
        each_depth(lambda step: wait_both(share_copy(sweep, step, True)))
        value = share_in[sweep, sink_depth]
        shared[sweep] = value
        full[sweep, my_core, my_depth] = value
        each_depth(lambda step: shared_copy(sweep, step, False).start())

    def sink_swap(sweep):
        each_depth(lambda step: wait_both(shared_copy(sweep, step, True)))
        swap_copy(sweep, False).start()

    def sink_end(sweep):
        copy = swap_copy(sweep, True)
        copy.wait_send()
        copy.wait_recv()

    def sink_sum():
        def one(step, sums):
            plane, chunk = step // 4, step % 4

            def rotation(sweep):
                fields = []
                for part in range(2):
                    for field in range(4):
                        tile = (plane * 4 + field) * 4 + chunk
                        fields.append(
                            full[
                                sweep,
                                part,
                                tile // 3,
                                pl.ds(pl.multiple_of(lax.rem(tile, 3) * 8, 8), 8),
                                :,
                            ]
                        )
                return rotation_of(fields)

            total = matrix_product(rotation(1), rotation(0))

            def source(part, pair):
                return pr[pl.ds((part * 6 + pair) * L + 16 * chunk + plane, 8, stride=2), :]

            out = list(sums)
            for group in range(2):
                column = [(source(0, group * 3 + c), source(1, group * 3 + c)) for c in range(3)]
                for a in range(3):
                    at = group * 3 + a
                    for c in range(3):
                        real, imag = c_mul(total[a][c], column[c])
                        out[at] = out[at] + real
                        out[6 + at] = out[6 + at] + imag
            return tuple(out)

        zero = jnp.zeros((8, 128), F32)
        sums = lax.fori_loop(0, 8, one, (zero,) * 12)
        for at in range(12):
            lines[at : at + 1, :] = jnp.sum(sums[at], axis=0, keepdims=True)

    def line_copy(step, arrival):
        peer = lax.rem(me + step, space_count)
        landing = peer if arrival else me
        return pltpu.make_async_remote_copy(
            src_ref=line,
            dst_ref=line_in.at[landing],
            send_sem=line_send.at[step],
            recv_sem=line_recv.at[landing],
            device_id={"space": peer},
            device_id_type=MESH,
        )

    def total_copy(step, arrival):
        peer = lax.rem(my_time + step, time_count)
        landing = peer if arrival else my_time
        return pltpu.make_async_remote_copy(
            src_ref=total_line,
            dst_ref=total_in.at[landing],
            send_sem=last_send.at[step],
            recv_sem=last_recv.at[landing],
            device_id={"tm": peer},
            device_id_type=MESH,
        )

    def over(count, action):
        def one(step, carry):
            action(step)
            return carry

        lax.fori_loop(1, count, one, 0)

    load_links.wait()
    spread(0)
    pl.semaphore_wait(barrier, space_count + time_count - 2)
    start_exchange(0)
    end_exchange(0)
    across(0)
    start_exchange(1)
    end_exchange(1)
    gather_back(0)
    sink_start(0)
    exponentials(0)
    rotate_links()
    spread(1)
    start_exchange(2)
    sink_shares(0)
    anchor_lines(0)
    end_exchange(2)
    across(1)
    start_exchange(3)
    sink_shared(0)
    end_exchange(3)
    gather_back(1)
    sink_start(1)
    sink_swap(0)
    exponentials(1)
    sink_shares(1)
    rotate_links()
    store_links = pltpu.make_async_copy(lk, links_out, copy_sem.at[0])
    store_links.start()
    sink_shared(1)
    anchor_lines(1)
    load_prop.wait()
    sink_end(0)
    sink_swap(1)
    sink_end(1)
    sink_sum()
    values = jnp.sum(lines[...], axis=1, keepdims=True)
    diagonal = lax.broadcasted_iota(jnp.int32, (48, 128), 0) == lax.broadcasted_iota(
        jnp.int32, (48, 128), 1
    )
    mine = jnp.sum(jnp.where(diagonal, values, 0.0), axis=0, keepdims=True)
    line[...] = mine
    over(space_count, lambda step: line_copy(step, False).start())
    line_in[me] = mine
    over(space_count, lambda step: wait_both(line_copy(step, True)))
    summed = jnp.sum(line_in[...], axis=0)
    total_line[...] = summed
    over(time_count, lambda step: total_copy(step, False).start())
    total_in[my_time] = summed
    over(time_count, lambda step: wait_both(total_copy(step, True)))
    rows_out[...] = total_in[...]
    store_links.wait()


def complex_matrix(parts):
    return parts.reshape(2, 3, 3)


def body(space_count, time_count, links, propagator, sink_time, src_time, src_site):
    planes = links.shape[5]

    def dense(values, count):
        folded = values.reshape(count, planes, ROWS, 128).transpose(0, 2, 1, 3)
        return folded.reshape(count * planes * ROWS, 128)

    link_rows = dense(links, 54)
    prop_rows = dense(propagator, 12)
    constants = [jnp.asarray(table) for table in tables(space_count)]
    smem = pl.BlockSpec(memory_space=pltpu.SMEM)
    vmem = pl.BlockSpec(memory_space=pltpu.VMEM)
    anywhere = pl.BlockSpec(memory_space=pl.ANY)
    dma = pltpu.SemaphoreType.DMA
    depth_count = time_count // 2
    fixed_rows, rows = pl.pallas_call(
        functools.partial(kernel, space_count, time_count),
        out_shape=(
            jax.ShapeDtypeStruct(link_rows.shape, F32),
            jax.ShapeDtypeStruct((time_count, 1, 128), F32),
        ),
        in_specs=[smem] * 3 + [anywhere] * 2 + [vmem] * 9,
        out_specs=(anywhere, vmem),
        scratch_shapes=[
            pltpu.VMEM(link_rows.shape, F32),
            pltpu.VMEM(prop_rows.shape, F32),
            pltpu.VMEM((4, space_count * PART, 128), F32),
            pltpu.VMEM((4, space_count * PART, 128), F32),
            pltpu.VMEM((2, 768, 128), F32),
            pltpu.VMEM((3, 18, ROWS, 128), F32),
            pltpu.VMEM((2, 18, ROWS, 128), F32),
            pltpu.VMEM((2, 256, 128), F32),
            pltpu.VMEM((2, depth_count, SHARE, 128), F32),
            pltpu.VMEM((2, depth_count, SHARE, 128), F32),
            pltpu.VMEM((2, SHARE, 128), F32),
            pltpu.VMEM((2, 2, depth_count, SHARE, 128), F32),
            pltpu.VMEM((48, 128), F32),
            pltpu.VMEM((1, 128), F32),
            pltpu.VMEM((space_count, 1, 128), F32),
            pltpu.VMEM((1, 128), F32),
            pltpu.VMEM((time_count, 1, 128), F32),
            dma((2,)),
            dma((4, space_count)),
            dma((4, space_count)),
            dma((2, 2)),
            dma((2, depth_count)),
            dma((2, depth_count)),
            dma((2, depth_count)),
            dma((2, depth_count)),
            dma((2, 2)),
            dma((space_count,)),
            dma((space_count,)),
            dma((time_count,)),
            dma((time_count,)),
        ],
        compiler_params=pltpu.CompilerParams(
            collective_id=0, has_side_effects=True, vmem_limit_bytes=48 * 1024 * 1024
        ),
    )(sink_time, src_time, src_site, link_rows, prop_rows, *constants)
    fixed = fixed_rows.reshape(54, ROWS, planes, 128).transpose(0, 2, 1, 3).reshape(links.shape)
    rows = rows.reshape(time_count, 128)
    sums = rows[:, :SC].reshape(time_count, 2, 6).transpose(1, 0, 2).reshape(2, 4, 3, SC)
    anchors = jnp.sum(rows[:, SC : SC + 36], axis=0)
    first, second = complex_matrix(anchors[:18]), complex_matrix(anchors[18:])

    def product(left, right):
        return jnp.sum(left[:, :, None] * right[None, :, :], axis=1)

    real = product(second[0], first[0]) - product(second[1], first[1])
    imag = product(second[0], first[1]) + product(second[1], first[0])

    def rotated(values, matrix):
        return jnp.sum(values[:, None] * matrix[None, :, :, None], axis=2)

    wall = jnp.stack(
        [
            rotated(sums[0], real) + rotated(sums[1], imag),
            rotated(sums[1], real) - rotated(sums[0], imag),
        ]
    ).reshape(2, SC * SC)
    return fixed, wall * float(planes * space_count * L * L) ** (-0.5)


def solution(mesh):
    placed = (
        P("tm", None, None, None, None, "space", None),
        P(None, "tm", "space", None),
        P(),
        P(),
        P(),
    )
    return jax.shard_map(
        functools.partial(body, mesh.shape["space"], mesh.shape["tm"]),
        mesh=mesh,
        in_specs=placed,
        out_specs=(P("tm", None, None, None, None, "space", None), P()),
        check_vma=False,
    )
```
